32 devices in a mesh: shard: 8 (over z, x), tp: 4 (over y, core).
Axes of the slice: x: 2, y: 2, z: 4, core: 2. Of those that a mesh axis runs over, the one named last changes fastest.
Arguments:
- one_gate: float32 [2048, 8192], P('shard', 'tp'), may hold values from -0.1875 to 0.1875
- other_gate: float32 [2048, 8192], P('shard', 'tp'), may hold values from -0.125 to 0.125
- one_up: float32 [2048, 8192], P('shard', 'tp'), may hold values from -0.1875 to 0.1875
- other_up: float32 [2048, 8192], P('shard', 'tp'), may hold values from -0.125 to 0.125
- mix_share: float32 [2048], P('shard'), may hold values from 0.2 to 0.8
- norm_train: float32 [2048], P(('shard', 'tp')), may hold values from 0.25 to 1.75
- norm_step: float32 [2048], P(('shard', 'tp')), may hold values from -0.3 to 0.3
Outputs:
- serve_gate: bfloat16 [2048, 8192], P(None, 'tp')
- serve_up: bfloat16 [2048, 8192], P(None, 'tp')
- factor_gate: float32 [8192], P('tp')
- factor_up: float32 [8192], P('tp')
- serve_norm: bfloat16 [2048], replicated
The draws below stay inside these ranges and needn't reach their ends.
All inputs are finite; a program needn't handle non-finite values.
Results may differ from the reference program's by a relative error of at most 0.0004.
Values may be sent and summed in bfloat16 or wider, within the bound.
A program may use at most 128 MiB of HBM per device.

```python
import jax
import jax.numpy as jnp
from jax import lax

D_MODEL = 2048
D_INNER = 8192


def with_spikes(array, key, source, target, blocks, factor):
    owner, partner = [(jnp.arange(array.shape[axis_at]) // (array.shape[axis_at] // blocks)).reshape([-1 if axis == axis_at else 1 for axis in range(array.ndim)]) for axis_at in (source, target)]
    chosen = jax.random.permutation(key, blocks)[partner]
    strong = (owner == chosen) | (owner == (partner + blocks // 2) % blocks)
    return jnp.where(strong, factor * array, array)


def shard_levels(key, shape, pieces, low, largest):
    level = 1.0
    for axis_at, shards_of in pieces:
        draws = jax.random.uniform(jax.random.fold_in(jax.random.fold_in(key, 6), axis_at), (shards_of,), jnp.float32, low / len(pieces), largest / len(pieces))
        level = level * jnp.repeat(jnp.exp(draws), shape[axis_at] // shards_of).reshape((-1,) + (1,) * (len(shape) - 1 - axis_at))
    return level


def normal_values(stream_key, extent, width, bound, split=(), kind=jnp.bfloat16):
    level = shard_levels(stream_key, extent, split, -0.22, 0.18) if split else 1.0
    values = jax.random.normal(stream_key, extent, jnp.float32) * width * level
    return jnp.minimum(jnp.maximum(values, -bound), bound).astype(kind)


def bell_draw_with(own_key, shape, width, most, split, heavy, held_as=jnp.bfloat16):
    result = width * jax.random.normal(own_key, shape, jnp.float32)
    if split:
        result = result * shard_levels(own_key, shape, split, -0.22, 0.18)
    return jnp.clip(with_spikes(result, jax.random.fold_in(own_key, 3), *heavy), -most, most).astype(held_as)


def setup_inputs(seed: int = 0) -> dict:
    arg_keys = jax.random.split(jax.random.key(seed), 8)
    one_gate = bell_draw_with(arg_keys[0], (D_MODEL, D_INNER), D_MODEL ** -0.5, 0.1875, ((0, 8), (1, 4)), (0, 1, 8, 2.0), jnp.float32)
    other_gate = normal_values(arg_keys[1], (D_MODEL, D_INNER), D_MODEL ** -0.5, 0.125, ((0, 8), (1, 4)), jnp.float32)
    one_up = bell_draw_with(arg_keys[2], (D_MODEL, D_INNER), D_MODEL ** -0.5, 0.1875, ((0, 8), (1, 4)), (0, 1, 8, 2.0), jnp.float32)
    other_up = normal_values(arg_keys[3], (D_MODEL, D_INNER), D_MODEL ** -0.5, 0.125, ((0, 8), (1, 4)), jnp.float32)
    mix_share = jnp.clip(0.2 + 0.6 * jax.random.uniform(arg_keys[4], (D_MODEL,), jnp.float32) ** shard_levels(arg_keys[4], (D_MODEL,), ((0, 8),), -0.2, 0.2), 0.2, 0.8)
    norm_train = jnp.clip(1.0 + 0.15 * jax.random.normal(arg_keys[5], (D_MODEL,), jnp.float32), 0.25, 1.75)
    norm_step = jnp.clip(jax.random.uniform(arg_keys[6], (D_MODEL,), jnp.float32, -0.3, 0.3) * shard_levels(arg_keys[6], (D_MODEL,), ((0, 32),), -0.4, 0.0), -0.3, 0.3)
    return dict(one_gate=one_gate, other_gate=other_gate, one_up=one_up, other_up=other_up, mix_share=mix_share, norm_train=norm_train, norm_step=norm_step)


def reference(one_gate, other_gate, one_up, other_up, mix_share, norm_train, norm_step):
    fresh_gate = mix_share[:, None] * one_gate + (1.0 - mix_share[:, None]) * other_gate
    fresh_up = mix_share[:, None] * one_up + (1.0 - mix_share[:, None]) * other_up
    factor_gate = jnp.sqrt(lax.optimization_barrier(jnp.sum(fresh_gate * fresh_gate, axis=0)))
    serve_gate = (fresh_gate / factor_gate).astype(jnp.bfloat16)
    factor_up = jnp.sqrt(lax.optimization_barrier(jnp.sum(fresh_up * fresh_up, axis=0)))
    serve_up = (fresh_up / factor_up).astype(jnp.bfloat16)
    serve_norm = (norm_train + norm_step).astype(jnp.bfloat16)
    return (serve_gate, serve_up, factor_gate, factor_up, serve_norm)
```

```python
import functools

import jax
import jax.numpy as jnp
from jax import lax
from jax.experimental import pallas as pl
from jax.experimental.pallas import tpu as pltpu
from jax.sharding import PartitionSpec as P

MESH = pl.DeviceIdType.MESH
UP, DOWN, ACROSS = 0, 1, 2


def gather_kernel(
    n, parts, pieces, one_gate, other_gate, one_up, other_up, mix, train, step,
    held, factor, norm,
    ones, others, sums, in_sem, sum_send, sum_recv, norm_send, norm_recv, send_sem, recv_sem,
):
    me = lax.axis_index("shard")
    part = lax.axis_index("tp")
    m, half = n // 2, pieces // 2
    place, side = me // 2, me % 2
    rows, cols = ones.shape[1:]
    tall = rows // half

    def reads(piece):
        a, at = piece // half, pl.ds(piece % half * tall, tall)
        first, second = ((one_gate, other_gate), (one_up, other_up))[a]
        return (
            pltpu.make_async_copy(first.at[at], ones.at[a, at], in_sem.at[0, piece]),
            pltpu.make_async_copy(second.at[at], others.at[a, at], in_sem.at[1, piece]),
        )

    for piece in range(pieces):
        for copy in reads(piece):
            copy.start()

    barrier = pltpu.get_barrier_semaphore()

    @pl.loop(1, n)
    def _(off):
        pl.semaphore_signal(barrier, inc=1, device_id={"shard": lax.rem(me + off, n)}, device_id_type=MESH)

    @pl.loop(1, parts)
    def _(off):
        pl.semaphore_signal(barrier, inc=1, device_id={"tp": lax.rem(part + off, parts)}, device_id_type=MESH)

    pl.semaphore_wait(barrier, n + parts - 2)

    norm[me, part] = train[...] + step[...]

    def norm_row(off):
        return pltpu.make_async_remote_copy(
            src_ref=norm.at[me, part], dst_ref=norm.at[me, part],
            send_sem=norm_send.at[off], recv_sem=norm_recv.at[off],
            device_id={"tp": lax.rem(part + off, parts)}, device_id_type=MESH,
        )

    def norm_group(off):
        return pltpu.make_async_remote_copy(
            src_ref=norm.at[me], dst_ref=norm.at[me],
            send_sem=norm_send.at[parts + off], recv_sem=norm_recv.at[parts + off],
            device_id={"shard": lax.rem(me + off, n)}, device_id_type=MESH,
        )

    @pl.loop(1, parts)
    def _(off):
        norm_row(off).start()

    for a in range(2):
        total = jnp.zeros((8, cols), jnp.float32)
        for piece in range(a * half, (a + 1) * half):
            for copy in reads(piece):
                copy.wait()

            def mixed(r, total):
                at = pl.ds(pl.multiple_of(piece % half * tall + r * 8, 8), 8)
                share = mix[at]
                fresh = share * ones[a, at] + (1.0 - share) * others[a, at]
                ones[a, at] = fresh
                return total + fresh * fresh

            total = lax.fori_loop(0, tall // 8, mixed, total)
        sums[me, pl.ds(a, 1)] = jnp.sum(total, axis=0, keepdims=True)

    def sum_copy(off):
        return pltpu.make_async_remote_copy(
            src_ref=sums.at[me], dst_ref=sums.at[me],
            send_sem=sum_send.at[off], recv_sem=sum_recv.at[off],
            device_id={"shard": lax.rem(me + off, n)}, device_id_type=MESH,
        )

    @pl.loop(1, n)
    def _(off):
        sum_copy(off).start()

    @pl.loop(1, parts)
    def _(off):
        norm_row(off).wait()

    @pl.loop(1, n)
    def _(off):
        norm_group(off).start()

    @pl.loop(1, n)
    def _(off):
        sum_copy(off).wait_recv()

    factors = jnp.sqrt(lax.fori_loop(1, n, lambda i, t: t + sums[i], sums[0]))
    factor[...] = factors
    scales = 1.0 / factors

    def piece_of(j, s, c):
        at = pl.multiple_of((2 * j + s) * rows + c % half * tall, 8)
        return held.at[c // half, pl.ds(at, tall)]

    def send(way, j, s, c, slot=None):
        target = {
            UP: {"shard": lax.rem(me + 2, n)},
            DOWN: {"shard": lax.rem(me + n - 2, n)},
            ACROSS: {"shard": 2 * place + 1 - side},
        }[way]
        block = piece_of(j, s, c)
        return pltpu.make_async_remote_copy(
            src_ref=block, dst_ref=block,
            send_sem=send_sem.at[way * m + j if slot is None else slot, c],
            recv_sem=recv_sem.at[2 * j + s, c],
            device_id=target, device_id_type=MESH,
        )

    def arrived(j, s, c):
        block = piece_of(j, s, c)
        pltpu.make_async_copy(block, block, recv_sem.at[2 * j + s, c]).wait()

    last = m - 1
    first_place, last_place = place == 0, place == last

    def crosses(j, c):
        kept = (first_place & (j == 1)) | (last_place & (j == last - 1))
        kept = kept & (c >= half)
        return ~(kept | ((place == 1) & (j == 0)) | ((place == last - 1) & (j == last)))

    for c in range(pieces):
        a, at = c // half, c % half * tall
        scale = scales[a : a + 1]

        def scaled(r, _):
            here = pl.multiple_of(at + r * 8, 8)
            there = pl.multiple_of(me * rows + at + r * 8, 8)
            held[a, pl.ds(there, 8)] = (ones[a, pl.ds(here, 8)] * scale).astype(jnp.bfloat16)
            return 0

        lax.fori_loop(0, tall // 8, scaled, 0)

        @pl.when(~last_place)
        def _():
            send(UP, place, side, c).start()

        @pl.when(~first_place)
        def _():
            send(DOWN, place, side, c).start()

        send(ACROSS, place, side, c).start()

    extra = 3 * m

    def ends(b, c):
        return (first_place | last_place) & (b == 1)

    def inner(b, c):
        return ((place == 1) | (place == last - 1)) & (b == last - 1) & (c >= half)

    @pl.loop(0, last * pieces)
    def _(slot):
        b, c = slot // pieces, slot % pieces

        @pl.when(b < place)
        def _():
            j = place - 1 - b
            arrived(j, side, c)

            @pl.when(~last_place)
            def _():
                send(UP, j, side, c).start()

            @pl.when(crosses(j, c))
            def _():
                send(ACROSS, j, side, c).start()

        @pl.when(b < last - place)
        def _():
            j = place + 1 + b
            arrived(j, side, c)

            @pl.when(~first_place)
            def _():
                send(DOWN, j, side, c).start()

            @pl.when(crosses(j, c))
            def _():
                send(ACROSS, j, side, c).start()

        @pl.when(ends(b, c) | inner(b, c))
        def _():
            arrived(place, 1 - side, c)

            @pl.when(first_place | (place == last - 1))
            def _():
                send(UP, place, 1 - side, c, extra).start()

            @pl.when(last_place | (place == 1))
            def _():
                send(DOWN, place, 1 - side, c, extra).start()

    @pl.loop(0, m * pieces)
    def _(slot):
        j, c = slot // pieces, slot % pieces
        passed_on = first_place | last_place | (((place == 1) | (place == last - 1)) & (c >= half))

        @pl.when(~((j == place) & passed_on))
        def _():
            arrived(j, 1 - side, c)

        @pl.when((j <= place) & ~last_place)
        def _():
            send(UP, j, side, c).wait_send()

        @pl.when((j >= place) & ~first_place)
        def _():
            send(DOWN, j, side, c).wait_send()

        @pl.when(crosses(j, c))
        def _():
            send(ACROSS, j, side, c).wait_send()

        @pl.when((j == place) & passed_on)
        def _():
            send(UP, place, 1 - side, c, extra).wait_send()

    @pl.loop(1, n)
    def _(off):
        sum_copy(off).wait_send()
        norm_group(off).wait()


def write_kernel(n, held, gate, up, sem):
    rows = held.shape[1] // n
    copies = [
        pltpu.make_async_copy(held.at[a, pl.ds(i * rows, rows)], out.at[pl.ds(i * rows, rows)], sem.at[a, i])
        for i in range(n)
        for a, out in enumerate((gate, up))
    ]
    for copy in copies:
        copy.start()
    for copy in copies:
        copy.wait()


def shards(n, parts, one_gate, other_gate, one_up, other_up, mix_share, norm_train, norm_step):
    rows, cols = one_gate.shape
    few = norm_train.shape[0]
    pieces = 2 * max(1, rows // 64)
    kinds = pltpu.SemaphoreType
    vmem, anywhere = pl.BlockSpec(memory_space=pltpu.VMEM), pl.BlockSpec(memory_space=pl.ANY)
    held, factors, norm = pl.pallas_call(
        functools.partial(gather_kernel, n, parts, pieces),
        out_shape=(
            pltpu.VMEM((2, n * rows, cols), jnp.bfloat16),
            jax.ShapeDtypeStruct((2, cols), jnp.float32),
            jax.ShapeDtypeStruct((n, parts, 1, few), jnp.float32),
        ),
        in_specs=[anywhere] * 4 + [vmem] * 3,
        out_specs=(vmem, vmem, vmem),
        scratch_shapes=[
            pltpu.VMEM((2, rows, cols), jnp.float32),
            pltpu.VMEM((2, rows, cols), jnp.float32),
            pltpu.VMEM((n, 2, cols), jnp.float32),
            kinds.DMA((2, pieces)),
            kinds.DMA((n,)),
            kinds.DMA((n,)),
            kinds.DMA((n + parts,)),
            kinds.DMA((n + parts,)),
            kinds.DMA((3 * (n // 2) + 1, pieces)),
            kinds.DMA((n, pieces)),
        ],
        compiler_params=pltpu.CompilerParams(
            collective_id=0, has_side_effects=True, vmem_limit_bytes=36 * 2**20
        ),
        name="mix_gather",
    )(
        one_gate, other_gate, one_up, other_up, mix_share[:, None],
        norm_train[None], norm_step[None],
    )
    gate, up = pl.pallas_call(
        functools.partial(write_kernel, n),
        out_shape=(jax.ShapeDtypeStruct((n * rows, cols), jnp.bfloat16),) * 2,
        in_specs=[vmem],
        out_specs=(anywhere, anywhere),
        scratch_shapes=[kinds.DMA((2, n))],
        compiler_params=pltpu.CompilerParams(vmem_limit_bytes=20 * 2**20),
        name="write_out",
    )(held)
    return gate, up, factors[0], factors[1], norm.reshape(-1).astype(jnp.bfloat16)


def solution(mesh):
    return jax.shard_map(
        functools.partial(shards, mesh.shape["shard"], mesh.shape["tp"]),
        mesh=mesh,
        in_specs=(
            P("shard", "tp"),
            P("shard", "tp"),
            P("shard", "tp"),
            P("shard", "tp"),
            P("shard"),
            P(("shard", "tp")),
            P(("shard", "tp")),
        ),
        out_specs=(P(None, "tp"), P(None, "tp"), P("tp"), P("tp"), P()),
        check_vma=False,
    )
```

```python
import functools

import jax
import jax.numpy as jnp
from jax import lax
from jax.experimental import pallas as pl
from jax.experimental.pallas import tpu as pltpu
from jax.sharding import PartitionSpec as P

MESH = pl.DeviceIdType.MESH
UP, DOWN, ACROSS = 0, 1, 2


def gather_kernel(
    n, parts, pieces, one_gate, other_gate, one_up, other_up, mix, train, step,
    held, factor_gate, factor_up, norm,
    ones, others, sums, mix_row, shares, gains, in_sem, small_sem,
    sum_send, sum_recv, norm_send, norm_recv, send_sem, recv_sem,
):
    me = lax.axis_index("shard")
    part = lax.axis_index("tp")
    m, half = n // 2, pieces // 2
    place, side = me // 2, me % 2
    rows, cols = ones.shape[1:]
    tall = rows // half
    lanes = shares.shape[1]

    barrier = pltpu.get_barrier_semaphore()

    @pl.loop(1, n)
    def _(off):
        pl.semaphore_signal(barrier, inc=1, device_id={"shard": lax.rem(me + off, n)}, device_id_type=MESH)

    @pl.loop(1, parts)
    def _(off):
        pl.semaphore_signal(barrier, inc=1, device_id={"tp": lax.rem(part + off, parts)}, device_id_type=MESH)

    read_mix = pltpu.make_async_copy(mix, mix_row, small_sem.at[0])
    read_gains = [
        pltpu.make_async_copy(source, gains.at[i], small_sem.at[1 + i]) for i, source in enumerate((train, step))
    ]

    def reads(piece):
        a, at = piece // half, pl.ds(piece % half * tall, tall)
        first, second = ((one_gate, other_gate), (one_up, other_up))[a]
        return (
            pltpu.make_async_copy(first.at[at], ones.at[a, at], in_sem.at[0, piece]),
            pltpu.make_async_copy(second.at[at], others.at[a, at], in_sem.at[1, piece]),
        )

    read_mix.start()
    for piece in range(pieces):
        for copy in reads(piece):
            copy.start()
    for copy in read_gains:
        copy.start()
    read_mix.wait()
    shares[...] = jnp.transpose(jnp.broadcast_to(mix_row[...], (lanes, shares.shape[0])))

    def mix_and_sum(a):
        total = jnp.zeros((8, cols), jnp.float32)
        for piece in range(a * half, (a + 1) * half):
            for copy in reads(piece):
                copy.wait()

            def mixed(r, total):
                at = pl.ds(pl.multiple_of(piece % half * tall + r * 8, 8), 8)
                share = shares[at]
                rest = 1.0 - share
                share, rest = (jnp.concatenate([v] * (cols // lanes), axis=1) for v in (share, rest))
                fresh = share * ones[a, at] + rest * others[a, at]
                ones[a, at] = fresh
                return total + fresh * fresh

            total = lax.fori_loop(0, tall // 8, mixed, total, unroll=2)
        sums[a, me] = jnp.sum(total, axis=0, keepdims=True)

    def sum_copy(a, off):
        return pltpu.make_async_remote_copy(
            src_ref=sums.at[a, me], dst_ref=sums.at[a, me],
            send_sem=sum_send.at[a, off], recv_sem=sum_recv.at[a, off],
            device_id={"shard": lax.rem(me + off, n)}, device_id_type=MESH,
        )

    def exchange(a):
        @pl.loop(1, n)
        def _(off):
            sum_copy(a, off).start()

    def scales(a):
        @pl.loop(1, n)
        def _(off):
            sum_copy(a, off).wait_recv()

        factors = jnp.sqrt(lax.fori_loop(1, n, lambda i, t: t + sums[a, i], sums[a, 0]))
        (factor_gate, factor_up)[a][...] = factors
        return jnp.broadcast_to(1.0 / factors, (8, cols))

    def norm_row(off):
        return pltpu.make_async_remote_copy(
            src_ref=norm.at[me, part], dst_ref=norm.at[me, part],
            send_sem=norm_send.at[off], recv_sem=norm_recv.at[off],
            device_id={"tp": lax.rem(part + off, parts)}, device_id_type=MESH,
        )

    def norm_group(off):
        return pltpu.make_async_remote_copy(
            src_ref=norm.at[me], dst_ref=norm.at[me],
            send_sem=norm_send.at[parts + off], recv_sem=norm_recv.at[parts + off],
            device_id={"shard": lax.rem(me + off, n)}, device_id_type=MESH,
        )

    def piece_of(j, s, c):
        at = pl.multiple_of((2 * j + s) * rows + c % half * tall, 8)
        return held.at[c // half, pl.ds(at, tall)]

    def send(way, j, s, c, slot=None):
        target = {
            UP: {"shard": lax.rem(me + 2, n)},
            DOWN: {"shard": lax.rem(me + n - 2, n)},
            ACROSS: {"shard": 2 * place + 1 - side},
        }[way]
        block = piece_of(j, s, c)
        return pltpu.make_async_remote_copy(
            src_ref=block, dst_ref=block,
            send_sem=send_sem.at[way * m + j if slot is None else slot, c],
            recv_sem=recv_sem.at[2 * j + s, c],
            device_id=target, device_id_type=MESH,
        )

    def arrived(j, s, c):
        block = piece_of(j, s, c)
        pltpu.make_async_copy(block, block, recv_sem.at[2 * j + s, c]).wait()

    last = m - 1
    first_place, last_place = place == 0, place == last

    def crosses(j, c):
        kept = (first_place & (j == 1)) | (last_place & (j == last - 1))
        kept = kept & (c >= half)
        return ~(kept | ((place == 1) & (j == 0)) | ((place == last - 1) & (j == last)))

    def own(a):
        scale = scales(a)
        for c in range(a * half, (a + 1) * half):
            at = c % half * tall

            def scaled(r, _):
                here = pl.multiple_of(at + r * 8, 8)
                there = pl.multiple_of(me * rows + at + r * 8, 8)
                held[a, pl.ds(there, 8)] = (ones[a, pl.ds(here, 8)] * scale).astype(jnp.bfloat16)
                return 0

            lax.fori_loop(0, tall // 8, scaled, 0, unroll=2)

            @pl.when(~last_place)
            def _():
                send(UP, place, side, c).start()

            @pl.when(~first_place)
            def _():
                send(DOWN, place, side, c).start()

            send(ACROSS, place, side, c).start()

    mix_and_sum(0)
    pl.semaphore_wait(barrier, n + parts - 2)
    exchange(0)
    own(0)
    for copy in read_gains:
        copy.wait()
    norm[me, part] = gains[0] + gains[1]

    @pl.loop(1, parts)
    def _(off):
        norm_row(off).start()

    mix_and_sum(1)
    exchange(1)

    @pl.loop(1, parts)
    def _(off):
        norm_row(off).wait()

    @pl.loop(1, n)
    def _(off):
        norm_group(off).start()

    own(1)
    extra = 3 * m

    def ends(b, c):
        return (first_place | last_place) & (b == 1)

    def inner(b, c):
        return ((place == 1) | (place == last - 1)) & (b == last - 1) & (c >= half)

    @pl.loop(0, last * pieces)
    def _(slot):
        b, c = slot // pieces, slot % pieces

        @pl.when(b < place)
        def _():
            j = place - 1 - b
            arrived(j, side, c)

            @pl.when(~last_place)
            def _():
                send(UP, j, side, c).start()

            @pl.when(crosses(j, c))
            def _():
                send(ACROSS, j, side, c).start()

        @pl.when(b < last - place)
        def _():
            j = place + 1 + b
            arrived(j, side, c)

            @pl.when(~first_place)
            def _():
                send(DOWN, j, side, c).start()

            @pl.when(crosses(j, c))
            def _():
                send(ACROSS, j, side, c).start()

        @pl.when(ends(b, c) | inner(b, c))
        def _():
            arrived(place, 1 - side, c)

            @pl.when(first_place | (place == last - 1))
            def _():
                send(UP, place, 1 - side, c, extra).start()

            @pl.when(last_place | (place == 1))
            def _():
                send(DOWN, place, 1 - side, c, extra).start()

    @pl.loop(0, m * pieces)
    def _(slot):
        j, c = slot // pieces, slot % pieces
        passed_on = first_place | last_place | (((place == 1) | (place == last - 1)) & (c >= half))

        @pl.when(~((j == place) & passed_on))
        def _():
            arrived(j, 1 - side, c)

        @pl.when((j <= place) & ~last_place)
        def _():
            send(UP, j, side, c).wait_send()

        @pl.when((j >= place) & ~first_place)
        def _():
            send(DOWN, j, side, c).wait_send()

        @pl.when(crosses(j, c))
        def _():
            send(ACROSS, j, side, c).wait_send()

        @pl.when((j == place) & passed_on)
        def _():
            send(UP, place, 1 - side, c, extra).wait_send()

    @pl.loop(1, n)
    def _(off):
        sum_copy(0, off).wait_send()
        sum_copy(1, off).wait_send()
        norm_group(off).wait()


def write_kernel(n, held, factor_gate, factor_up, gate, up, out_gate, out_up, sem, small_sem):
    rows = held.shape[1] // n
    copies = [
        pltpu.make_async_copy(held.at[a, pl.ds(i * rows, rows)], out.at[pl.ds(i * rows, rows)], sem.at[a, i])
        for i in range(n)
        for a, out in enumerate((gate, up))
    ]
    copies.append(pltpu.make_async_copy(factor_gate, out_gate, small_sem.at[0]))
    copies.append(pltpu.make_async_copy(factor_up, out_up, small_sem.at[1]))
    for copy in copies:
        copy.start()
    for copy in copies:
        copy.wait()


def shards(n, parts, one_gate, other_gate, one_up, other_up, mix_share, norm_train, norm_step):
    rows, cols = one_gate.shape
    few = norm_train.shape[0]
    lanes = 128
    padded = -(-rows // lanes) * lanes
    pieces = 2 * max(1, rows // 64)
    kinds = pltpu.SemaphoreType
    vmem, anywhere = pl.BlockSpec(memory_space=pltpu.VMEM), pl.BlockSpec(memory_space=pl.ANY)
    held, factor_gate, factor_up, norm = pl.pallas_call(
        functools.partial(gather_kernel, n, parts, pieces),
        out_shape=(
            pltpu.VMEM((2, n * rows, cols), jnp.bfloat16),
            pltpu.VMEM((1, cols), jnp.float32),
            pltpu.VMEM((1, cols), jnp.float32),
            pltpu.VMEM((n, parts, 1, few), jnp.float32),
        ),
        in_specs=[pl.BlockSpec(memory_space=pltpu.HBM)] * 7,
        out_specs=(vmem,) * 4,
        scratch_shapes=[
            pltpu.VMEM((2, rows, cols), jnp.float32),
            pltpu.VMEM((2, rows, cols), jnp.float32),
            pltpu.VMEM((2, n, 1, cols), jnp.float32),
            pltpu.VMEM((1, padded), jnp.float32),
            pltpu.VMEM((padded, lanes), jnp.float32),
            pltpu.VMEM((2, 1, few), jnp.float32),
            kinds.DMA((2, pieces)),
            kinds.DMA((3,)),
            kinds.DMA((2, n)),
            kinds.DMA((2, n)),
            kinds.DMA((n + parts,)),
            kinds.DMA((n + parts,)),
            kinds.DMA((3 * (n // 2) + 1, pieces)),
            kinds.DMA((n, pieces)),
        ],
        compiler_params=pltpu.CompilerParams(
            collective_id=0, has_side_effects=True, vmem_limit_bytes=46 * 2**20
        ),
        name="mix_gather",
    )(
        one_gate, other_gate, one_up, other_up,
        jnp.pad(mix_share, (0, padded - rows))[None], norm_train[None], norm_step[None],
    )
    gate, up, factor_gate, factor_up = pl.pallas_call(
        functools.partial(write_kernel, n),
        out_shape=(jax.ShapeDtypeStruct((n * rows, cols), jnp.bfloat16),) * 2
        + (jax.ShapeDtypeStruct((1, cols), jnp.float32),) * 2,
        in_specs=[vmem] * 3,
        out_specs=(anywhere,) * 4,
        scratch_shapes=[kinds.DMA((2, n)), kinds.DMA((2,))],
        compiler_params=pltpu.CompilerParams(vmem_limit_bytes=2**20),
        name="write_out",
    )(held, factor_gate, factor_up)
    return gate, up, factor_gate[0], factor_up[0], norm.reshape(-1).astype(jnp.bfloat16)


def solution(mesh):
    return jax.shard_map(
        functools.partial(shards, mesh.shape["shard"], mesh.shape["tp"]),
        mesh=mesh,
        in_specs=(
            P("shard", "tp"),
            P("shard", "tp"),
            P("shard", "tp"),
            P("shard", "tp"),
            P("shard"),
            P(("shard", "tp")),
            P(("shard", "tp")),
        ),
        out_specs=(P(None, "tp"), P(None, "tp"), P("tp"), P("tp"), P()),
        check_vma=False,
    )
```

```python
import functools

import jax
import jax.numpy as jnp
from jax import lax
from jax.experimental import pallas as pl
from jax.experimental.pallas import tpu as pltpu
from jax.sharding import PartitionSpec as P

MESH = pl.DeviceIdType.MESH
UP, DOWN, ACROSS = 0, 1, 2


def gather_kernel(
    n, parts, pieces, one_gate, other_gate, one_up, other_up, mix, train, step,
    held, factor_gate, factor_up, norm,
    ones, others, sums, mix_row, shares, gains, in_sem, small_sem,
    sum_send, sum_recv, norm_send, norm_recv, send_sem, recv_sem,
):
    me = lax.axis_index("shard")
    part = lax.axis_index("tp")
    m, half = n // 2, pieces // 2
    place, side = me // 2, me % 2
    rows, cols = ones.shape[1:]
    tall = rows // half
    lanes = shares.shape[1]

    barrier = pltpu.get_barrier_semaphore()

    @pl.loop(1, n)
    def _(off):
        pl.semaphore_signal(barrier, inc=1, device_id={"shard": lax.rem(me + off, n)}, device_id_type=MESH)

    @pl.loop(1, parts)
    def _(off):
        pl.semaphore_signal(barrier, inc=1, device_id={"tp": lax.rem(part + off, parts)}, device_id_type=MESH)

    read_mix = pltpu.make_async_copy(mix, mix_row, small_sem.at[0])
    read_gains = [
        pltpu.make_async_copy(source, gains.at[i], small_sem.at[1 + i]) for i, source in enumerate((train, step))
    ]

    def reads(piece):
        a, at = piece // half, pl.ds(piece % half * tall, tall)
        first, second = ((one_gate, other_gate), (one_up, other_up))[a]
        return (
            pltpu.make_async_copy(first.at[at], ones.at[a, at], in_sem.at[0, piece]),
            pltpu.make_async_copy(second.at[at], others.at[a, at], in_sem.at[1, piece]),
        )

    read_mix.start()
    for piece in range(half):
        for copy in reads(piece):
            copy.start()
    read_mix.wait()
    shares[...] = jnp.transpose(jnp.broadcast_to(mix_row[...], (lanes, shares.shape[0])))

    def mix_and_sum(a):
        total = jnp.zeros((8, cols), jnp.float32)
        for piece in range(a * half, (a + 1) * half):
            for copy in reads(piece):
                copy.wait()

            def mixed(r, total):
                at = pl.ds(pl.multiple_of(piece % half * tall + r * 8, 8), 8)
                share = shares[at]
                rest = 1.0 - share
                share, rest = (jnp.concatenate([v] * (cols // lanes), axis=1) for v in (share, rest))
                fresh = share * ones[a, at] + rest * others[a, at]
                ones[a, at] = fresh
                return total + fresh * fresh

            total = lax.fori_loop(0, tall // 8, mixed, total, unroll=4)
        sums[a, me] = jnp.sum(total, axis=0, keepdims=True)

    def sum_copy(a, off):
        return pltpu.make_async_remote_copy(
            src_ref=sums.at[a, me], dst_ref=sums.at[a, me],
            send_sem=sum_send.at[a, off], recv_sem=sum_recv.at[a, off],
            device_id={"shard": lax.rem(me + off, n)}, device_id_type=MESH,
        )

    def exchange(a):
        @pl.loop(1, n)
        def _(off):
            sum_copy(a, off).start()

    def scales(a):
        @pl.loop(1, n)
        def _(off):
            sum_copy(a, off).wait_recv()

        factors = jnp.sqrt(lax.fori_loop(1, n, lambda i, t: t + sums[a, i], sums[a, 0]))
        (factor_gate, factor_up)[a][...] = factors
        return jnp.broadcast_to(1.0 / factors, (8, cols))

    def norm_row(off):
        return pltpu.make_async_remote_copy(
            src_ref=norm.at[me, part], dst_ref=norm.at[me, part],
            send_sem=norm_send.at[off], recv_sem=norm_recv.at[off],
            device_id={"tp": lax.rem(part + off, parts)}, device_id_type=MESH,
        )

    def norm_group(off):
        return pltpu.make_async_remote_copy(
            src_ref=norm.at[me], dst_ref=norm.at[me],
            send_sem=norm_send.at[parts + off], recv_sem=norm_recv.at[parts + off],
            device_id={"shard": lax.rem(me + off, n)}, device_id_type=MESH,
        )

    def piece_of(j, s, c):
        at = pl.multiple_of((2 * j + s) * rows + c % half * tall, 8)
        return held.at[c // half, pl.ds(at, tall)]

    def send(way, j, s, c, slot=None):
        target = {
            UP: {"shard": lax.rem(me + 2, n)},
            DOWN: {"shard": lax.rem(me + n - 2, n)},
            ACROSS: {"shard": 2 * place + 1 - side},
        }[way]
        block = piece_of(j, s, c)
        return pltpu.make_async_remote_copy(
            src_ref=block, dst_ref=block,
            send_sem=send_sem.at[way * m + j if slot is None else slot, c],
            recv_sem=recv_sem.at[2 * j + s, c],
            device_id=target, device_id_type=MESH,
        )

    def arrived(j, s, c):
        block = piece_of(j, s, c)
        pltpu.make_async_copy(block, block, recv_sem.at[2 * j + s, c]).wait()

    last = m - 1
    first_place, last_place = place == 0, place == last

    def crosses(j, c):
        kept = (first_place & (j == 1)) | (last_place & (j == last - 1))
        kept = kept & (c >= half)
        return ~(kept | ((place == 1) & (j == 0)) | ((place == last - 1) & (j == last)))

    def own(a):
        scale = scales(a)
        for c in range(a * half, (a + 1) * half):
            at = c % half * tall

            def scaled(r, _):
                here = pl.multiple_of(at + r * 8, 8)
                there = pl.multiple_of(me * rows + at + r * 8, 8)
                held[a, pl.ds(there, 8)] = (ones[a, pl.ds(here, 8)] * scale).astype(jnp.bfloat16)
                return 0

            lax.fori_loop(0, tall // 8, scaled, 0, unroll=4)

            @pl.when(~last_place)
            def _():
                send(UP, place, side, c).start()

            @pl.when(~first_place)
            def _():
                send(DOWN, place, side, c).start()

            send(ACROSS, place, side, c).start()

    mix_and_sum(0)
    pl.semaphore_wait(barrier, n + parts - 2)
    exchange(0)
    for piece in range(half, pieces):
        for copy in reads(piece):
            copy.start()
    for copy in read_gains:
        copy.start()
    own(0)
    for copy in read_gains:
        copy.wait()
    norm[me, part] = gains[0] + gains[1]

    @pl.loop(1, parts)
    def _(off):
        norm_row(off).start()

    mix_and_sum(1)
    exchange(1)

    @pl.loop(1, parts)
    def _(off):
        norm_row(off).wait()

    @pl.loop(1, n)
    def _(off):
        norm_group(off).start()

    own(1)
    extra = 3 * m

    def ends(b, c):
        return (first_place | last_place) & (b == 1)

    def inner(b, c):
        return ((place == 1) | (place == last - 1)) & (b == last - 1) & (c >= half)

    @pl.loop(0, last * pieces)
    def _(slot):
        b, c = slot // pieces, slot % pieces

        @pl.when(b < place)
        def _():
            j = place - 1 - b
            arrived(j, side, c)

            @pl.when(~last_place)
            def _():
                send(UP, j, side, c).start()

            @pl.when(crosses(j, c))
            def _():
                send(ACROSS, j, side, c).start()

        @pl.when(b < last - place)
        def _():
            j = place + 1 + b
            arrived(j, side, c)

            @pl.when(~first_place)
            def _():
                send(DOWN, j, side, c).start()

            @pl.when(crosses(j, c))
            def _():
                send(ACROSS, j, side, c).start()

        @pl.when(ends(b, c) | inner(b, c))
        def _():
            arrived(place, 1 - side, c)

            @pl.when(first_place | (place == last - 1))
            def _():
                send(UP, place, 1 - side, c, extra).start()

            @pl.when(last_place | (place == 1))
            def _():
                send(DOWN, place, 1 - side, c, extra).start()

    passed_on = first_place | last_place
    passed_half = (place == 1) | (place == last - 1)
    inward = jnp.where(first_place, 1, last - 1)

    @pl.loop(1, n)
    def _(off):
        sum_copy(0, off).wait_send()
        sum_copy(1, off).wait_send()
        norm_group(off).wait()

    @pl.loop(0, m * pieces)
    def _(slot):
        b, c = slot // pieces, slot % pieces
        j = jnp.where(2 * place < last, b, last - b)
        passed = (j == place) & (passed_on | (passed_half & (c >= half)))
        late = passed_on & (j == inward) & (c >= half)

        @pl.when((j <= place) & ~last_place)
        def _():
            send(UP, j, side, c).wait_send()

        @pl.when((j >= place) & ~first_place)
        def _():
            send(DOWN, j, side, c).wait_send()

        @pl.when(passed)
        def _():
            send(UP, place, 1 - side, c, extra).wait_send()

        @pl.when(crosses(j, c))
        def _():
            send(ACROSS, j, side, c).wait_send()

        @pl.when(~(passed | late))
        def _():
            arrived(j, 1 - side, c)

    @pl.when(passed_on)
    def _():
        for c in range(half, pieces):
            arrived(inward, 1 - side, c)


def write_kernel(n, held, factor_gate, factor_up, gate, up, out_gate, out_up, sem, small_sem):
    rows = held.shape[1] // n
    copies = [
        pltpu.make_async_copy(held.at[a, pl.ds(i * rows, rows)], out.at[pl.ds(i * rows, rows)], sem.at[a, i])
        for i in range(n)
        for a, out in enumerate((gate, up))
    ]
    copies.append(pltpu.make_async_copy(factor_gate, out_gate, small_sem.at[0]))
    copies.append(pltpu.make_async_copy(factor_up, out_up, small_sem.at[1]))
    for copy in copies:
        copy.start()
    for copy in copies:
        copy.wait()


def shards(n, parts, one_gate, other_gate, one_up, other_up, mix_share, norm_train, norm_step):
    rows, cols = one_gate.shape
    few = norm_train.shape[0]
    lanes = 128
    padded = -(-rows // lanes) * lanes
    pieces = 2 * max(1, rows // 64)
    kinds = pltpu.SemaphoreType
    vmem, anywhere = pl.BlockSpec(memory_space=pltpu.VMEM), pl.BlockSpec(memory_space=pl.ANY)
    held, factor_gate, factor_up, norm = pl.pallas_call(
        functools.partial(gather_kernel, n, parts, pieces),
        out_shape=(
            pltpu.VMEM((2, n * rows, cols), jnp.bfloat16),
            pltpu.VMEM((1, cols), jnp.float32),
            pltpu.VMEM((1, cols), jnp.float32),
            pltpu.VMEM((n, parts, 1, few), jnp.float32),
        ),
        in_specs=[pl.BlockSpec(memory_space=pltpu.HBM)] * 7,
        out_specs=(vmem,) * 4,
        scratch_shapes=[
            pltpu.VMEM((2, rows, cols), jnp.float32),
            pltpu.VMEM((2, rows, cols), jnp.float32),
            pltpu.VMEM((2, n, 1, cols), jnp.float32),
            pltpu.VMEM((1, padded), jnp.float32),
            pltpu.VMEM((padded, lanes), jnp.float32),
            pltpu.VMEM((2, 1, few), jnp.float32),
            kinds.DMA((2, pieces)),
            kinds.DMA((3,)),
            kinds.DMA((2, n)),
            kinds.DMA((2, n)),
            kinds.DMA((n + parts,)),
            kinds.DMA((n + parts,)),
            kinds.DMA((3 * (n // 2) + 1, pieces)),
            kinds.DMA((n, pieces)),
        ],
        compiler_params=pltpu.CompilerParams(
            collective_id=0, has_side_effects=True, vmem_limit_bytes=46 * 2**20
        ),
        name="mix_gather",
    )(
        one_gate, other_gate, one_up, other_up,
        jnp.pad(mix_share, (0, padded - rows))[None], norm_train[None], norm_step[None],
    )
    gate, up, factor_gate, factor_up = pl.pallas_call(
        functools.partial(write_kernel, n),
        out_shape=(jax.ShapeDtypeStruct((n * rows, cols), jnp.bfloat16),) * 2
        + (jax.ShapeDtypeStruct((1, cols), jnp.float32),) * 2,
        in_specs=[vmem] * 3,
        out_specs=(anywhere,) * 4,
        scratch_shapes=[kinds.DMA((2, n)), kinds.DMA((2,))],
        compiler_params=pltpu.CompilerParams(vmem_limit_bytes=2**20),
        name="write_out",
    )(held, factor_gate, factor_up)
    return gate, up, factor_gate[0], factor_up[0], norm.reshape(-1).astype(jnp.bfloat16)


def solution(mesh):
    return jax.shard_map(
        functools.partial(shards, mesh.shape["shard"], mesh.shape["tp"]),
        mesh=mesh,
        in_specs=(
            P("shard", "tp"),
            P("shard", "tp"),
            P("shard", "tp"),
            P("shard", "tp"),
            P("shard"),
            P(("shard", "tp")),
            P(("shard", "tp")),
        ),
        out_specs=(P(None, "tp"), P(None, "tp"), P("tp"), P("tp"), P()),
        check_vma=False,
    )
```
